512 devices in a mesh: row: 16 (over z, core), col: 32 (over y, x).
Axes of the slice: x: 4, y: 8, z: 8, core: 2. Of those that a mesh axis runs over, the one named last changes fastest.
Arguments:
- weight: float32 [3584, 18432], P('row', 'col'), may hold values from -6 to 6
- momentum: float32 [3584, 18432], P('row', 'col'), may hold values from -6 to 6
- gradients: float32 [2, 3584, 18432], P(None, 'row', 'col'), may hold values from -6 to 6
- basis: float32 [18432, 256], P('col'), may hold values from -6 to 6
- step: int32 [1], replicated, may hold values from 0 to 63
Outputs:
- new_weight: float32 [3584, 18432], P('row', 'col')
- new_momentum: float32 [3584, 18432], P('row', 'col')
- new_basis: float32 [18432, 256], P('col')
The draws below stay inside these ranges and needn't reach their ends.
All inputs are finite; a program needn't handle non-finite values.
Results may differ from the reference program's by a relative error of at most 0.0004.
Values sent between devices are 32-bit elements; how exact they have to be, the bound alone decides.
A program may use at most 64 MiB of HBM per device.

```python
import jax
import jax.numpy as jnp
from jax import lax

DOUT = 3584
DIN = 18432
RANK = 256
STEPS = 2


def steps_of(own_key, shape, cuts, low, high):
    level, own = 1.0, jax.random.fold_in(own_key, 6)
    for axis_at, parts in cuts:
        steps = jnp.exp(jax.random.uniform(jax.random.fold_in(own, axis_at), (parts,), jnp.float32, low / len(cuts), high / len(cuts)))
        level = level * jnp.repeat(steps, shape[axis_at] // parts).reshape([-1 if axis == axis_at else 1 for axis in range(len(shape))])
    return level


def gaussian(key, shape, deviation, bound, split=(), held_as=jnp.bfloat16):
    gain = steps_of(key, shape, split, -0.22, 0.18) if split else 1.0
    entries = jax.random.normal(key, shape, jnp.float32) * deviation * gain
    return jnp.minimum(jnp.maximum(entries, -bound), bound).astype(held_as)


def setup_inputs(seed: int = 0) -> dict:
    streams_of = jax.random.split(jax.random.key(seed), 6)
    return {
        "weight": gaussian(streams_of[0], (DOUT, DIN), 1.0, 6.0, ((0, 16), (1, 32)), jnp.float32),
        "momentum": gaussian(streams_of[1], (DOUT, DIN), 1.0, 6.0, ((0, 16), (1, 32)), jnp.float32),
        "gradients": gaussian(streams_of[2], (STEPS, DOUT, DIN), 1.0, 6.0, ((1, 16), (2, 32)), jnp.float32),
        "basis": gaussian(streams_of[3], (DIN, RANK), 1.0, 6.0, ((0, 32),), jnp.float32),
        "step": jax.random.randint(streams_of[4], (1,), 0, 64).astype(jnp.int32),
    }


def matmul(left, right):
    return jnp.dot(left.astype(jnp.float32), right.astype(jnp.float32), precision=lax.Precision.HIGHEST, preferred_element_type=jnp.float32)

def reference(weight, momentum, gradients, basis, step):
    start = step[0]
    for index in range(STEPS):
        rate = 0.5 * jnp.minimum(1.0, (start + index + 1).astype(jnp.float32) / 64.0)
        buffer = momentum + gradients[index]
        panel = matmul(buffer, basis)
        gram = matmul(panel.T, panel)
        lower = jnp.linalg.cholesky(gram)
        ortho = jax.scipy.linalg.solve_triangular(lower, panel.T, lower=True).T
        factor = matmul(buffer.T, ortho)
        momentum = buffer - 0.05 * matmul(ortho, factor.T)
        scale = jnp.sqrt(lax.optimization_barrier(jnp.mean(factor * factor, axis=0)) + 1e-06)
        basis = factor / scale
        weight = weight - rate * jnp.sqrt(DOUT / RANK) * matmul(ortho, basis.T)
    return (weight, momentum, basis)
```

```python
import functools

import jax
import jax.numpy as jnp
from jax import lax
from jax.experimental import pallas as pl
from jax.experimental.pallas import tpu as pltpu
from jax.sharding import PartitionSpec as P

F32 = jnp.float32
BF16 = jnp.bfloat16
LANES = 128
PIVOTS = 16
NN = (((1,), (0,)), ((), ()))
NT = (((1,), (1,)), ((), ()))
TN = (((0,), (0,)), ((), ()))


def exact(left, right, dims):
    return lax.dot_general(left, right, dims, precision=lax.Precision.HIGHEST, preferred_element_type=F32)


def split(value):
    high = value.astype(BF16)
    return high, (value - high.astype(F32)).astype(BF16)


def product(left, right, dims):
    def dot(a, b):
        return lax.dot_general(a, b, dims, preferred_element_type=F32)

    return dot(left[0], right[0]) + (dot(left[0], right[1]) + dot(left[1], right[0]))


def eliminate(table, first, last):
    rank, width = table.shape
    rows = lax.broadcasted_iota(jnp.int32, (PIVOTS, LANES), 0)
    lanes = lax.broadcasted_iota(jnp.int32, (PIVOTS, rank), 1)

    def block(index, carry):
        start = pl.multiple_of(index * PIVOTS, PIVOTS)
        tile = pl.multiple_of((start // LANES) * LANES, LANES)
        corner = table[pl.ds(start, PIVOTS), pl.ds(tile, LANES)]
        corner = pltpu.roll(corner, lax.rem(LANES - lax.rem(start, LANES), LANES), 1)
        columns = [jnp.broadcast_to(corner[:, j : j + 1], (PIVOTS, LANES)) for j in range(PIVOTS)]
        parts = [table[pl.ds(start, PIVOTS), t * LANES : (t + 1) * LANES] for t in range(width // LANES)]
        for k in range(PIVOTS):
            inverse = lax.rsqrt(columns[k][k : k + 1, :])
            scaled = columns[k] * inverse
            below = jnp.where(rows > k, scaled, 0.0)
            for t, part in enumerate(parts):
                own = part[k : k + 1, :] * inverse
                parts[t] = jnp.where(rows == k, own, part - below * own)
            for j in range(k + 1, PIVOTS):
                columns[j] = columns[j] - below * scaled[j : j + 1, :]
        whole = jnp.concatenate(parts, axis=1)
        left = jnp.where(lanes >= start + PIVOTS, whole[:, :rank], 0.0)
        table[pl.ds(start, PIVOTS), :] = whole
        for r in range(0, rank, LANES):
            table[r : r + LANES, :] = table[r : r + LANES, :] - exact(left[:, r : r + LANES], whole, TN)
        return carry

    lax.fori_loop(first, last, block, 0)


def kernel(
    din, n_row, n_col, weight, momentum, gradients, basis, step, weight_out, momentum_out, basis_out,
    w, m, g, v, b, partial, panel_in, panel, gram, gram_in, gram_all, table, ortho,
    h_part, h_in, h_sum, h_rows, h_all, f, squares, load_sem, store_sem, send_sem, recv_sem,
):
    row, col = lax.axis_index("row"), lax.axis_index("col")
    core, z = lax.rem(row, 2), row // 2
    n_z = n_row // 2
    n_rows, n_cols = m.shape
    rank = v.shape[1]
    owned = panel_in.shape[2]
    owners = n_rows // owned
    strip = rank // n_col
    piece = n_cols // n_z
    half = rank // 2

    def on_col(other):
        return {"row": row, "col": other}

    def on_row(other):
        return {"row": other, "col": col}

    barrier = pltpu.get_barrier_semaphore()

    def greet_col(i, carry):
        pl.semaphore_signal(barrier, inc=1, device_id=on_col(lax.rem(col + i, n_col)))
        return carry

    def greet_row(i, carry):
        pl.semaphore_signal(barrier, inc=1, device_id=on_row(lax.rem(row + i, n_row)))
        return carry

    loads = [
        pltpu.make_async_copy(momentum, m, load_sem.at[0]),
        pltpu.make_async_copy(gradients, g, load_sem.at[1]),
        pltpu.make_async_copy(basis, v, load_sem.at[2]),
        pltpu.make_async_copy(weight, w, load_sem.at[3]),
    ]
    for load in loads:
        load.start()
    lax.fori_loop(1, n_col, greet_col, 0)
    lax.fori_loop(1, n_row, greet_row, 0)

    def remote(source, target, phase, s, device):
        return pltpu.make_async_remote_copy(
            src_ref=source, dst_ref=target, send_sem=send_sem.at[s, phase], recv_sem=recv_sem.at[s, phase],
            device_id=device, device_id_type=pl.DeviceIdType.MESH,
        )

    def arrived(block, phase, s):
        remote(block, block, phase, s, on_row(row + 1 - 2 * core)).wait_recv()

    def sent(block, phase, s):
        remote(block, block, phase, s, on_row(row + 1 - 2 * core)).wait_send()

    def to_cols(start):
        def body(i, carry):
            start(lax.rem(col + i, n_col))
            return carry

        lax.fori_loop(1, n_col, body, 0)

    def to_rows(start):
        def body(i, carry):
            start(lax.rem(row + i, n_row))
            return carry

        lax.fori_loop(1, n_row, body, 0)

    def to_layers(start):
        def body(i, carry):
            start(lax.rem(z + i, n_z))
            return carry

        lax.fori_loop(1, n_z, body, 0)

    for load in loads[:3]:
        load.wait()
    b[...] = m[...] + g[0]
    blocks = [(r, min(n_rows, r + 112)) for r in range(0, n_rows, 112)]
    for low, high in blocks:
        partial[0, low:high, :] = exact(b[low:high, :], v[...], NN)
    pl.semaphore_wait(barrier, n_col + n_row - 2)

    def panel_send(s):
        def start(other):
            @pl.when(other < owners)
            def _():
                remote(
                    partial.at[s, pl.ds(pl.multiple_of(other * owned, owned), owned)],
                    panel_in.at[s, col], 0, s, on_col(other),
                ).start()

        to_cols(start)

    def panel_finish(s):
        @pl.when(col < owners)
        def _():
            mine = pl.ds(pl.multiple_of(col * owned, owned), owned)
            panel_in[s, col] = partial[s, mine, :]
            arrived(panel_in.at[s, pl.ds(0, n_col - 1)], 0, s)
            panel[s, mine, :] = jnp.sum(panel_in[s], axis=0)

            def start(other):
                remote(panel.at[s, mine], panel.at[s, mine], 1, s, on_col(other)).start()

            to_cols(start)
            arrived(panel.at[s, pl.ds(0, (owners - 1) * owned)], 1, s)

        @pl.when(col >= owners)
        def _():
            arrived(panel.at[s], 1, s)

    def squares_send(s):
        squares[s, col] = jnp.sum(f[s] * f[s], axis=0, keepdims=True)

        def start(other):
            remote(squares.at[s, col], squares.at[s, col], 7, s, on_col(other)).start()

        to_cols(start)

    def scale_of(s):
        arrived(squares.at[s, pl.ds(0, n_col - 1)], 7, s)
        total = jnp.sum(squares[s], axis=0)
        return jnp.sqrt(total * (1.0 / din) + 1e-6)

    def weight_step(s, scale):
        rate = 0.5 * jnp.minimum(1.0, (step[0] + (s + 1)).astype(F32) / 64.0) * (n_rows * n_row / rank) ** 0.5
        right = split(f[s])
        for low, high in blocks:
            left = split(ortho[s, low:high, :] * (rate / scale))
            w[low:high, :] = w[low:high, :] - product(left, right, NT)

    panel_send(0)
    for s in range(2):
        if s == 1:
            squares_send(0)
            loads[3].wait()
            weight_step(0, scale_of(0))
        panel_finish(s)

        gram[s] = exact(panel[s], panel[s], TN)
        strip_here = pl.ds(pl.multiple_of(col * strip, strip), strip)

        def gram_send(other, s=s):
            remote(gram.at[s, strip_here], gram_in.at[s, row], 2, s, on_row(other)).start()

        to_rows(gram_send)
        gram_in[s, row] = gram[s, strip_here, :]

        for low in range(0, n_cols, LANES):
            high = min(n_cols, low + LANES)
            part = exact(b[:, low:high], panel[s], TN)
            for k in range(2):
                h_part[s, k, low:high, :] = part[:, k * half : (k + 1) * half]
        remote(h_part.at[s, 1 - core], h_in.at[s], 4, s, on_row(row + 1 - 2 * core)).start()

        arrived(gram_in.at[s, pl.ds(0, n_row - 1)], 2, s)
        gram_all[s, strip_here, :] = jnp.sum(gram_in[s], axis=0)

        def gram_share(other, s=s):
            remote(gram_all.at[s, strip_here], gram_all.at[s, strip_here], 3, s, on_col(other)).start()

        to_cols(gram_share)

        arrived(h_in.at[s], 4, s)
        h_sum[s] = h_part[s, core] + h_in[s]

        def piece_of(other):
            return pl.ds(pl.multiple_of(other * piece, 8), piece)

        def h_send(other, s=s):
            remote(h_sum.at[s, piece_of(other)], h_rows.at[s, z], 5, s, on_row(2 * other + core)).start()

        to_layers(h_send)
        h_rows[s, z] = h_sum[s, piece_of(z), :]

        arrived(gram_all.at[s, pl.ds(0, rank - strip)], 3, s)
        table[:, :rank] = gram_all[s]
        table[:, rank:] = jnp.where(
            lax.broadcasted_iota(jnp.int32, (rank, rank), 0) == lax.broadcasted_iota(jnp.int32, (rank, rank), 1), 1.0, 0.0
        )
        n_blocks = rank // PIVOTS
        eliminate(table, 0, n_blocks // 2)

        arrived(h_rows.at[s, pl.ds(0, n_z - 1)], 5, s)
        h_all[s, core, piece_of(z), :] = jnp.sum(h_rows[s], axis=0)

        def h_share(other, s=s):
            mine = h_all.at[s, core, piece_of(z)]
            remote(mine, mine, 6, s, on_row(2 * other + core)).start()

        to_layers(h_share)
        eliminate(table, n_blocks // 2, n_blocks)
        arrived(h_all.at[s, 0, pl.ds(0, n_cols - piece)], 6, s)
        remote(h_all.at[s, core], h_all.at[s, core], 8, s, on_row(row + 1 - 2 * core)).start()

        inverse = table[:, rank:]
        for low, high in blocks:
            ortho[s, low:high, :] = exact(panel[s, low:high, :], inverse, NT)
        arrived(h_all.at[s, 0], 8, s)
        for low in range(0, n_cols, 192):
            high = min(n_cols, low + 192)
            f[s, low:high, :] = exact(h_all[s, 0, low:high, :], inverse[:, :half], NT) + exact(
                h_all[s, 1, low:high, :], inverse[:, half:], NT
            )
        if s == 1:
            squares_send(1)
        right = split(f[s])
        for low, high in blocks:
            b[low:high, :] = b[low:high, :] - 0.05 * product(split(ortho[s, low:high, :]), right, NT)
            if s == 0:
                b[low:high, :] = b[low:high, :] + g[1, low:high, :]
                partial[1, low:high, :] = exact(b[low:high, :], f[0], NN)
        if s == 0:
            panel_send(1)

    stores = [
        pltpu.make_async_copy(b, momentum_out, store_sem.at[0]),
        pltpu.make_async_copy(w, weight_out, store_sem.at[1]),
        pltpu.make_async_copy(v, basis_out, store_sem.at[2]),
    ]
    stores[0].start()
    scale = scale_of(1)
    v[...] = f[1] / scale
    stores[2].start()
    weight_step(1, scale)
    stores[1].start()

    for s in range(2):
        @pl.when(col < owners)
        def _(s=s):
            sent(panel_in.at[s, pl.ds(0, owners - 1)], 0, s)
            sent(panel_in.at[s, pl.ds(0, n_col - 1)], 1, s)

        @pl.when(col >= owners)
        def _(s=s):
            sent(panel_in.at[s, pl.ds(0, owners)], 0, s)

        sent(gram_in.at[s, pl.ds(0, n_row - 1)], 2, s)
        sent(gram_all.at[s, pl.ds(0, rank - strip)], 3, s)
        sent(h_in.at[s], 4, s)
        sent(h_rows.at[s, pl.ds(0, n_z - 1)], 5, s)
        sent(h_rows.at[s, pl.ds(0, n_z - 1)], 6, s)
        sent(squares.at[s, pl.ds(0, n_col - 1)], 7, s)
        sent(h_in.at[s], 8, s)
    for store in stores:
        store.wait()


def solution(mesh):
    n_row, n_col = mesh.shape["row"], mesh.shape["col"]

    def local(weight, momentum, gradients, basis, step):
        (n_rows, n_cols), rank = weight.shape, basis.shape[1]
        owned = -(-n_rows // (8 * n_col)) * 8
        anywhere = pl.BlockSpec(memory_space=pl.ANY)
        vmem = functools.partial(pltpu.VMEM, dtype=F32)
        half, n_z = rank // 2, n_row // 2
        return pl.pallas_call(
            functools.partial(kernel, n_cols * n_col, n_row, n_col),
            out_shape=(
                jax.ShapeDtypeStruct(weight.shape, F32),
                jax.ShapeDtypeStruct(weight.shape, F32),
                jax.ShapeDtypeStruct(basis.shape, F32),
            ),
            in_specs=[anywhere] * 4 + [pl.BlockSpec(memory_space=pltpu.SMEM)],
            out_specs=(anywhere,) * 3,
            scratch_shapes=[
                vmem((n_rows, n_cols)),
                vmem((n_rows, n_cols)),
                vmem((2, n_rows, n_cols)),
                vmem((n_cols, rank)),
                vmem((n_rows, n_cols)),
                vmem((2, n_rows, rank)),
                vmem((2, n_col, owned, rank)),
                vmem((2, n_rows, rank)),
                vmem((2, rank, rank)),
                vmem((2, n_row, rank // n_col, rank)),
                vmem((2, rank, rank)),
                vmem((rank, 2 * rank)),
                vmem((2, n_rows, rank)),
                vmem((2, 2, n_cols, half)),
                vmem((2, n_cols, half)),
                vmem((2, n_cols, half)),
                vmem((2, n_z, n_cols // n_z, half)),
                vmem((2, 2, n_cols, half)),
                vmem((2, n_cols, rank)),
                vmem((2, n_col, 1, rank)),
                pltpu.SemaphoreType.DMA((4,)),
                pltpu.SemaphoreType.DMA((3,)),
                pltpu.SemaphoreType.DMA((2, 9)),
                pltpu.SemaphoreType.DMA((2, 9)),
            ],
            compiler_params=pltpu.CompilerParams(collective_id=0, has_side_effects=True, vmem_limit_bytes=60000 * 1024),
        )(weight, momentum, gradients, basis, step)

    return jax.shard_map(
        local,
        mesh=mesh,
        in_specs=(P("row", "col"), P("row", "col"), P(None, "row", "col"), P("col", None), P()),
        out_specs=(P("row", "col"), P("row", "col"), P("col", None)),
        check_vma=False,
    )
```

```python
import functools

import jax
import jax.numpy as jnp
from jax import lax
from jax.experimental import pallas as pl
from jax.experimental.pallas import tpu as pltpu
from jax.sharding import PartitionSpec as P

F32 = jnp.float32
BF16 = jnp.bfloat16
LANES = 128
PIVOTS = 32
NN = (((1,), (0,)), ((), ()))
NT = (((1,), (1,)), ((), ()))
TN = (((0,), (0,)), ((), ()))


def exact(left, right, dims):
    return lax.dot_general(left, right, dims, precision=lax.Precision.HIGHEST, preferred_element_type=F32)


def split(value):
    high = value.astype(BF16)
    return high, (value - high.astype(F32)).astype(BF16)


def product(left, right, dims):
    def dot(a, b):
        return lax.dot_general(a, b, dims, preferred_element_type=F32)

    return dot(left[0], right[0]) + (dot(left[0], right[1]) + dot(left[1], right[0]))


def eliminate(table, phase):
    rank = table.shape[0]
    tiles = PIVOTS // 8
    base = phase * LANES
    live = [base + k * LANES for k in range(3)]
    rows = lax.broadcasted_iota(jnp.int32, (8, LANES), 0)
    lanes = lax.broadcasted_iota(jnp.int32, (PIVOTS, LANES), 1)

    def block(index, carry):
        offset = pl.multiple_of(index * PIVOTS, PIVOTS)
        start = pl.multiple_of(base + offset, PIVOTS)
        corner = table[pl.ds(start, PIVOTS), base : base + LANES]
        corner = pltpu.roll(corner, lax.rem(LANES - offset, LANES), 1)
        column = {}
        for j in range(PIVOTS):
            for t in range(j // 8, tiles):
                column[t, j] = jnp.broadcast_to(corner[8 * t : 8 * t + 8, j : j + 1], (8, LANES))
        part = {
            (t, i): table[pl.ds(start + 8 * t, 8), lane : lane + LANES] for t in range(tiles) for i, lane in enumerate(live)
        }
        for k in range(PIVOTS):
            top, at = k // 8, k % 8
            inverse = lax.rsqrt(column[top, k][at : at + 1, :])
            scaled = [column[t, k] * inverse if t >= top else None for t in range(tiles)]
            below = list(scaled)
            below[top] = jnp.where(rows > at, scaled[top], 0.0)
            for j in range(k + 1, PIVOTS):
                weight = scaled[j // 8][j % 8 : j % 8 + 1, :]
                for t in range(j // 8, tiles):
                    column[t, j] = column[t, j] - below[t] * weight
            for i in range(len(live)):
                own = part[top, i][at : at + 1, :] * inverse
                for t in range(top, tiles):
                    part[t, i] = part[t, i] - below[t] * own
                part[top, i] = jnp.where(rows == at, own, part[top, i])
        strips = [jnp.concatenate([part[t, i] for t in range(tiles)], axis=0) for i in range(len(live))]
        for i, lane in enumerate(live):
            table[pl.ds(start, PIVOTS), lane : lane + LANES] = strips[i]
        for r in range(phase, rank // LANES):
            left = strips[r - phase]
            if r == phase:
                left = jnp.where(lanes >= offset + PIVOTS, left, 0.0)
            first = 0 if r == phase else 1
            change = exact(left, jnp.concatenate(strips[first:], axis=1), TN)
            region = (slice(r * LANES, (r + 1) * LANES), slice(live[first], live[-1] + LANES))
            table[region] = table[region] - change
        return carry

    lax.fori_loop(0, LANES // PIVOTS, block, 0)


def kernel(
    din, n_row, n_col, weight, momentum, gradients, basis, step, weight_out, momentum_out, basis_out,
    w, m, g, v, b, partial, panel_in, panel, gram, gram_in, gram_all, table, ortho,
    h_part, h_in, h_sum, h_rows, h_all, f, squares, load_sem, send_sem, recv_sem,
):
    row, col = lax.axis_index("row"), lax.axis_index("col")
    core, z = lax.rem(row, 2), row // 2
    n_z = n_row // 2
    n_rows, n_cols = m.shape
    rank = v.shape[1]
    owned = panel_in.shape[2]
    owners = n_rows // owned
    strip = rank // n_col
    piece = n_cols // n_z
    half = rank // 2

    def on_col(other):
        return {"row": row, "col": other}

    def on_row(other):
        return {"row": other, "col": col}

    barrier = pltpu.get_barrier_semaphore()

    def greet_col(i, carry):
        pl.semaphore_signal(barrier, inc=1, device_id=on_col(lax.rem(col + i, n_col)))
        return carry

    def greet_row(i, carry):
        pl.semaphore_signal(barrier, inc=1, device_id=on_row(lax.rem(row + i, n_row)))
        return carry

    loads = [
        pltpu.make_async_copy(momentum, m, load_sem.at[0]),
        pltpu.make_async_copy(gradients, g, load_sem.at[1]),
        pltpu.make_async_copy(basis, v, load_sem.at[2]),
        pltpu.make_async_copy(weight, w, load_sem.at[3]),
    ]
    for load in loads:
        load.start()
    lax.fori_loop(1, n_col, greet_col, 0)
    lax.fori_loop(1, n_row, greet_row, 0)

    def remote(source, target, phase, s, device):
        return pltpu.make_async_remote_copy(
            src_ref=source, dst_ref=target, send_sem=send_sem.at[s, phase], recv_sem=recv_sem.at[s, phase],
            device_id=device, device_id_type=pl.DeviceIdType.MESH,
        )

    def arrived(block, phase, s):
        remote(block, block, phase, s, on_row(row + 1 - 2 * core)).wait_recv()

    def sent(block, phase, s):
        remote(block, block, phase, s, on_row(row + 1 - 2 * core)).wait_send()

    def to_cols(start):
        def body(i, carry):
            start(lax.rem(col + i, n_col))
            return carry

        lax.fori_loop(1, n_col, body, 0)

    def to_rows(start):
        def body(i, carry):
            start(lax.rem(row + i, n_row))
            return carry

        lax.fori_loop(1, n_row, body, 0)

    def to_layers(start):
        def body(i, carry):
            start(lax.rem(z + i, n_z))
            return carry

        lax.fori_loop(1, n_z, body, 0)

    for load in loads[:3]:
        load.wait()
    b[...] = m[...] + g[0]
    blocks = [(r, min(n_rows, r + 112)) for r in range(0, n_rows, 112)]
    start = split(v[...])
    for low, high in blocks:
        partial[0, low:high, :] = product(split(b[low:high, :]), start, NN)
    pl.semaphore_wait(barrier, n_col + n_row - 2)

    def panel_send(s):
        def start(other):
            @pl.when(other < owners)
            def _():
                remote(
                    partial.at[s, pl.ds(pl.multiple_of(other * owned, owned), owned)],
                    panel_in.at[s, col], 0, s, on_col(other),
                ).start()

        to_cols(start)

    def panel_finish(s):
        @pl.when(col < owners)
        def _():
            mine = pl.ds(pl.multiple_of(col * owned, owned), owned)
            panel_in[s, col] = partial[s, mine, :]
            arrived(panel_in.at[s, pl.ds(0, n_col - 1)], 0, s)
            panel[s, mine, :] = jnp.sum(panel_in[s], axis=0)

            def start(other):
                remote(panel.at[s, mine], panel.at[s, mine], 1, s, on_col(other)).start()

            to_cols(start)
            arrived(panel.at[s, pl.ds(0, (owners - 1) * owned)], 1, s)

        @pl.when(col >= owners)
        def _():
            arrived(panel.at[s], 1, s)

    def squares_send(s):
        squares[s, col] = jnp.sum(f[s] * f[s], axis=0, keepdims=True)

        def start(other):
            remote(squares.at[s, col], squares.at[s, col], 7, s, on_col(other)).start()

        to_cols(start)

    def scale_of(s):
        arrived(squares.at[s, pl.ds(0, n_col - 1)], 7, s)
        total = jnp.sum(squares[s], axis=0)
        return jnp.sqrt(total * (1.0 / din) + 1e-6)

    def weight_step(s, scale):
        rate = 0.5 * jnp.minimum(1.0, (step[0] + (s + 1)).astype(F32) / 64.0) * (n_rows * n_row / rank) ** 0.5
        right = split(f[s])
        for low, high in blocks:
            left = split(ortho[s, low:high, :] * (rate / scale))
            w[low:high, :] = w[low:high, :] - product(left, right, NT)

    panel_send(0)
    for s in range(2):
        if s == 1:
            squares_send(0)
            loads[3].wait()
            weight_step(0, scale_of(0))
        panel_finish(s)

        gram[s] = exact(panel[s], panel[s], TN)
        strip_here = pl.ds(pl.multiple_of(col * strip, strip), strip)

        def gram_send(other, s=s):
            remote(gram.at[s, strip_here], gram_in.at[s, row], 2, s, on_row(other)).start()

        to_rows(gram_send)
        gram_in[s, row] = gram[s, strip_here, :]

        panel_parts = split(panel[s])
        for low in range(0, n_cols, LANES):
            high = min(n_cols, low + LANES)
            part = product(split(b[:, low:high]), panel_parts, TN)
            for k in range(2):
                h_part[s, k, low:high, :] = part[:, k * half : (k + 1) * half]
        remote(h_part.at[s, 1 - core], h_in.at[s], 4, s, on_row(row + 1 - 2 * core)).start()

        def piece_of(other):
            return pl.ds(pl.multiple_of(other * piece, 8), piece)

        def h_send(other, s=s):
            remote(h_sum.at[s, piece_of(other)], h_rows.at[s, z], 5, s, on_row(2 * other + core)).start()

        def h_share(other, s=s):
            mine = h_all.at[s, core, piece_of(z)]
            remote(mine, mine, 6, s, on_row(2 * other + core)).start()

        upper = col < n_col // 2
        right = pl.ds(half, half)

        def gram_share(other, s=s):
            @pl.when(upper)
            def _():
                remote(gram_all.at[s, strip_here], gram_all.at[s, strip_here], 3, s, on_col(other)).start()

            @pl.when(jnp.logical_not(upper))
            def _():
                mine = gram_all.at[s, strip_here, right]
                remote(mine, mine, 9, s, on_col(other)).start()

        arrived(h_in.at[s], 4, s)
        h_sum[s] = h_part[s, core] + h_in[s]
        to_layers(h_send)
        h_rows[s, z] = h_sum[s, piece_of(z), :]

        arrived(gram_in.at[s, pl.ds(0, n_row - 1)], 2, s)
        gram_all[s, strip_here, :] = jnp.sum(gram_in[s], axis=0)
        to_cols(gram_share)

        table[:, rank:] = jnp.where(
            lax.broadcasted_iota(jnp.int32, (rank, rank), 0) == lax.broadcasted_iota(jnp.int32, (rank, rank), 1), 1.0, 0.0
        )
        arrived(h_rows.at[s, pl.ds(0, n_z - 1)], 5, s)
        h_all[s, core, piece_of(z), :] = jnp.sum(h_rows[s], axis=0)
        to_layers(h_share)

        @pl.when(upper)
        def _(s=s):
            arrived(gram_all.at[s, pl.ds(0, half - strip)], 3, s)
            arrived(gram_all.at[s, pl.ds(0, half), right], 9, s)

        @pl.when(jnp.logical_not(upper))
        def _(s=s):
            arrived(gram_all.at[s, pl.ds(0, half)], 3, s)
            arrived(gram_all.at[s, pl.ds(0, half - strip), right], 9, s)

        table[:half, :rank] = gram_all[s, :half, :]
        table[half:, half:rank] = gram_all[s, half:, half:]
        eliminate(table, 0)
        eliminate(table, 1)
        arrived(h_all.at[s, 0, pl.ds(0, n_cols - piece)], 6, s)
        remote(h_all.at[s, core], h_all.at[s, core], 8, s, on_row(row + 1 - 2 * core)).start()

        inverse = split(table[:, rank:])
        for low, high in blocks:
            ortho[s, low:high, :] = product(split(panel[s, low:high, :]), inverse, NT)
        arrived(h_all.at[s, 0], 8, s)
        for low in range(0, n_cols, 192):
            high = min(n_cols, low + 192)
            f[s, low:high, :] = sum(
                product(split(h_all[s, k, low:high, :]), [x[:, k * half : (k + 1) * half] for x in inverse], NT) for k in range(2)
            )
        if s == 1:
            squares_send(1)
        right = split(f[s])
        for low, high in blocks:
            b[low:high, :] = b[low:high, :] - 0.05 * product(split(ortho[s, low:high, :]), right, NT)
            if s == 0:
                b[low:high, :] = b[low:high, :] + g[1, low:high, :]
                partial[1, low:high, :] = product(split(b[low:high, :]), right, NN)
        if s == 0:
            panel_send(1)

    momentum_out[...] = b[...]
    scale = scale_of(1)
    basis_out[...] = f[1] / scale
    weight_step(1, scale)
    weight_out[...] = w[...]

    for s in range(2):
        @pl.when(col < owners)
        def _(s=s):
            sent(panel_in.at[s, pl.ds(0, owners - 1)], 0, s)
            sent(panel_in.at[s, pl.ds(0, n_col - 1)], 1, s)

        @pl.when(col >= owners)
        def _(s=s):
            sent(panel_in.at[s, pl.ds(0, owners)], 0, s)

        sent(gram_in.at[s, pl.ds(0, n_row - 1)], 2, s)

        @pl.when(col < n_col // 2)
        def _(s=s):
            sent(gram_all.at[s, pl.ds(0, (n_col - 1) * strip)], 3, s)

        @pl.when(col >= n_col // 2)
        def _(s=s):
            sent(gram_all.at[s, pl.ds(0, (n_col - 1) * strip), pl.ds(half, half)], 9, s)

        sent(h_in.at[s], 4, s)
        sent(h_rows.at[s, pl.ds(0, n_z - 1)], 5, s)
        sent(h_rows.at[s, pl.ds(0, n_z - 1)], 6, s)
        sent(squares.at[s, pl.ds(0, n_col - 1)], 7, s)
        sent(h_in.at[s], 8, s)


def solution(mesh):
    n_row, n_col = mesh.shape["row"], mesh.shape["col"]

    def local(weight, momentum, gradients, basis, step):
        (n_rows, n_cols), rank = weight.shape, basis.shape[1]
        owned = -(-n_rows // (8 * n_col)) * 8
        anywhere = pl.BlockSpec(memory_space=pltpu.HBM)
        vmem = functools.partial(pltpu.VMEM, dtype=F32)
        half, n_z = rank // 2, n_row // 2
        return pl.pallas_call(
            functools.partial(kernel, n_cols * n_col, n_row, n_col),
            out_shape=(
                jax.ShapeDtypeStruct(weight.shape, F32),
                jax.ShapeDtypeStruct(weight.shape, F32),
                jax.ShapeDtypeStruct(basis.shape, F32),
            ),
            in_specs=[anywhere] * 4 + [pl.BlockSpec(memory_space=pltpu.SMEM)],
            out_specs=(pl.BlockSpec(memory_space=pltpu.VMEM),) * 3,
            scratch_shapes=[
                vmem((n_rows, n_cols)),
                vmem((n_rows, n_cols)),
                vmem((2, n_rows, n_cols)),
                vmem((n_cols, rank)),
                vmem((n_rows, n_cols)),
                vmem((2, n_rows, rank)),
                vmem((2, n_col, owned, rank)),
                vmem((2, n_rows, rank)),
                vmem((2, rank, rank)),
                vmem((2, n_row, rank // n_col, rank)),
                vmem((2, rank, rank)),
                vmem((rank, 2 * rank)),
                vmem((2, n_rows, rank)),
                vmem((2, 2, n_cols, half)),
                vmem((2, n_cols, half)),
                vmem((2, n_cols, half)),
                vmem((2, n_z, n_cols // n_z, half)),
                vmem((2, 2, n_cols, half)),
                vmem((2, n_cols, rank)),
                vmem((2, n_col, 1, rank)),
                pltpu.SemaphoreType.DMA((4,)),
                pltpu.SemaphoreType.DMA((2, 10)),
                pltpu.SemaphoreType.DMA((2, 10)),
            ],
            compiler_params=pltpu.CompilerParams(collective_id=0, has_side_effects=True, vmem_limit_bytes=54500 * 1024),
        )(weight, momentum, gradients, basis, step)

    return jax.shard_map(
        local,
        mesh=mesh,
        in_specs=(P("row", "col"), P("row", "col"), P(None, "row", "col"), P("col", None), P()),
        out_specs=(P("row", "col"), P("row", "col"), P("col", None)),
        check_vma=False,
    )
```

```python
import functools

import jax
import jax.numpy as jnp
from jax import lax
from jax.experimental import pallas as pl
from jax.experimental.pallas import tpu as pltpu
from jax.sharding import PartitionSpec as P

F32 = jnp.float32
BF16 = jnp.bfloat16
LANES = 128
PIVOTS = 32
NN = (((1,), (0,)), ((), ()))
NT = (((1,), (1,)), ((), ()))
TN = (((0,), (0,)), ((), ()))


def exact(left, right, dims):
    return lax.dot_general(left, right, dims, precision=lax.Precision.HIGHEST, preferred_element_type=F32)


def split(value):
    high = value.astype(BF16)
    return high, (value - high.astype(F32)).astype(BF16)


def product(left, right, dims):
    def dot(a, b):
        return lax.dot_general(a, b, dims, preferred_element_type=F32)

    return dot(left[0], right[0]) + (dot(left[0], right[1]) + dot(left[1], right[0]))


def stacked(left, right):
    def thirds(value):
        high, rest = value.astype(BF16), value - value.astype(BF16).astype(F32)
        middle = rest.astype(BF16)
        return high, middle, (rest - middle.astype(F32)).astype(BF16)

    a, b = thirds(left), thirds(right)
    pairs = ((0, 2), (2, 0), (1, 1), (0, 1), (1, 0), (0, 0))
    return lax.dot_general(
        jnp.concatenate([a[i] for i, _ in pairs], axis=0),
        jnp.concatenate([b[j] for _, j in pairs], axis=0),
        TN,
        preferred_element_type=F32,
    )


def eliminate(table, phase):
    rank = table.shape[0]
    tiles = PIVOTS // 8
    base = phase * LANES
    live = [base + k * LANES for k in range(3)]
    rows = lax.broadcasted_iota(jnp.int32, (8, LANES), 0)
    lanes = lax.broadcasted_iota(jnp.int32, (PIVOTS, LANES), 1)

    def block(index, carry):
        offset = pl.multiple_of(index * PIVOTS, PIVOTS)
        start = pl.multiple_of(base + offset, PIVOTS)
        corner = table[pl.ds(start, PIVOTS), base : base + LANES]
        column = {}
        for j in range(PIVOTS):
            for t in range(j // 8, tiles):
                column[t, j] = jnp.take_along_axis(
                    corner[8 * t : 8 * t + 8, :], jnp.full((8, LANES), offset + j, jnp.int32), axis=1, mode="promise_in_bounds"
                )
        part = {
            (t, i): table[pl.ds(start + 8 * t, 8), lane : lane + LANES] for t in range(tiles) for i, lane in enumerate(live)
        }
        for k in range(PIVOTS):
            top, at = k // 8, k % 8
            inverse = lax.rsqrt(column[top, k][at : at + 1, :])
            scaled = [column[t, k] * inverse if t >= top else None for t in range(tiles)]
            below = list(scaled)
            below[top] = jnp.where(rows > at, scaled[top], 0.0)
            for j in range(k + 1, PIVOTS):
                weight = scaled[j // 8][j % 8 : j % 8 + 1, :]
                for t in range(j // 8, tiles):
                    column[t, j] = column[t, j] - below[t] * weight
            for i in range(len(live)):
                own = part[top, i][at : at + 1, :] * inverse
                for t in range(top, tiles):
                    part[t, i] = part[t, i] - below[t] * own
                part[top, i] = jnp.where(rows == at, own, part[top, i])
        strips = [jnp.concatenate([part[t, i] for t in range(tiles)], axis=0) for i in range(len(live))]
        for i, lane in enumerate(live):
            table[pl.ds(start, PIVOTS), lane : lane + LANES] = strips[i]
        for r in range(phase, rank // LANES):
            left = strips[r - phase]
            if r == phase:
                left = jnp.where(lanes >= offset + PIVOTS, left, 0.0)
            first = 0 if r == phase else 1
            change = stacked(left, jnp.concatenate(strips[first:], axis=1))
            region = (slice(r * LANES, (r + 1) * LANES), slice(live[first], live[-1] + LANES))
            table[region] = table[region] - change
        return carry

    lax.fori_loop(0, LANES // PIVOTS, block, 0)


def kernel(
    din, n_row, n_col, weight, momentum, gradients, basis, step, weight_out, momentum_out, basis_out,
    w, m, g, v, b, partial, panel_in, panel, gram, gram_in, gram_all, table, ortho,
    h_part, h_in, h_sum, h_rows, h_all, f, squares, load_sem, send_sem, recv_sem,
):
    row, col = lax.axis_index("row"), lax.axis_index("col")
    core, z = lax.rem(row, 2), row // 2
    n_z = n_row // 2
    n_rows, n_cols = m.shape
    rank = v.shape[1]
    owned = panel_in.shape[2]
    owners = n_rows // owned
    strip = rank // n_col
    piece = n_cols // n_z
    half = rank // 2

    def on_col(other):
        return {"row": row, "col": other}

    def on_row(other):
        return {"row": other, "col": col}

    def others(me, count, act):
        for i in range(count - 1):
            away = count // 2 + ((i + 1) // 2) * (1 - 2 * (i % 2))
            act(jnp.where(me + away >= count, me + (away - count), me + away))

    barrier = pltpu.get_barrier_semaphore()

    def greet_col(other):
        pl.semaphore_signal(barrier, inc=1, device_id=on_col(other))

    def greet_row(other):
        pl.semaphore_signal(barrier, inc=1, device_id=on_row(other))

    loads = [
        pltpu.make_async_copy(momentum, m, load_sem.at[0]),
        pltpu.make_async_copy(gradients.at[0], g.at[0], load_sem.at[1]),
        pltpu.make_async_copy(basis, v, load_sem.at[2]),
        pltpu.make_async_copy(weight, w, load_sem.at[3]),
        pltpu.make_async_copy(gradients.at[1], g.at[1], load_sem.at[4]),
    ]
    for load in loads[:3]:
        load.start()
    others(col, n_col, greet_col)
    others(row, n_row, greet_row)

    def remote(source, target, phase, s, device):
        return pltpu.make_async_remote_copy(
            src_ref=source, dst_ref=target, send_sem=send_sem.at[s, phase], recv_sem=recv_sem.at[s, phase],
            device_id=device, device_id_type=pl.DeviceIdType.MESH,
        )

    def arrived(block, phase, s):
        remote(block, block, phase, s, on_row(row + 1 - 2 * core)).wait_recv()

    def sent(block, phase, s):
        remote(block, block, phase, s, on_row(row + 1 - 2 * core)).wait_send()

    for load in loads[:3]:
        load.wait()
    for load in loads[3:]:
        load.start()
    b[...] = m[...] + g[0]
    blocks = [(r, min(n_rows, r + 112)) for r in range(0, n_rows, 112)]
    start = split(v[...])
    for low, high in blocks:
        partial[0, low:high, :] = product(split(b[low:high, :]), start, NN)
    pl.semaphore_wait(barrier, n_col + n_row - 2)

    sides = [pl.ds(k * half, half) for k in range(2)]
    panel_phases = ((0, 1), (11, 12))

    def panel_send(s):
        for side, (phase, _) in zip(sides, panel_phases):

            def start(other, side=side, phase=phase):
                @pl.when(other < owners)
                def _():
                    remote(
                        partial.at[s, pl.ds(pl.multiple_of(other * owned, owned), owned), side],
                        panel_in.at[s, col, :, side], phase, s, on_col(other),
                    ).start()

            others(col, n_col, start)

    def panel_finish(s, meanwhile):
        @pl.when(col < owners)
        def _():
            mine = pl.ds(pl.multiple_of(col * owned, owned), owned)
            panel_in[s, col] = partial[s, mine, :]
            for side, (arrival, spread) in zip(sides, panel_phases):
                arrived(panel_in.at[s, pl.ds(0, n_col - 1), :, side], arrival, s)
                panel[s, mine, side] = jnp.sum(panel_in[s, :, :, side], axis=0)

                def start(other, side=side, spread=spread):
                    block = panel.at[s, mine, side]
                    remote(block, block, spread, s, on_col(other)).start()

                others(col, n_col, start)

        meanwhile()
        for side, (_, spread) in zip(sides, panel_phases):

            @pl.when(col < owners)
            def _(side=side, spread=spread):
                arrived(panel.at[s, pl.ds(0, (owners - 1) * owned), side], spread, s)

            @pl.when(col >= owners)
            def _(side=side, spread=spread):
                arrived(panel.at[s, :, side], spread, s)

    def squares_send(s):
        squares[s, col] = jnp.sum(f[s] * f[s], axis=0, keepdims=True)

        def start(other):
            remote(squares.at[s, col], squares.at[s, col], 7, s, on_col(other)).start()

        others(col, n_col, start)

    def scale_of(s):
        arrived(squares.at[s, pl.ds(0, n_col - 1)], 7, s)
        total = jnp.sum(squares[s], axis=0)
        return 1.0 / jnp.sqrt(total * (1.0 / din) + 1e-6)

    def weight_step(target, s, scale, right):
        rate = 0.5 * jnp.minimum(1.0, (step[0] + (s + 1)).astype(F32) / 64.0) * (n_rows * n_row / rank) ** 0.5
        for low, high in blocks:
            left = split(ortho[s, low:high, :] * (rate * scale))
            target[low:high, :] = w[low:high, :] - product(left, right, NT)

    panel_send(0)
    for s in range(2):
        if s == 1:
            squares_send(0)

        def meanwhile(s=s):
            if s == 1:
                weight_step(w, 0, scale_of(0), split(f[0]))
            else:
                for load in loads[3:]:
                    load.wait()

        panel_finish(s, meanwhile)

        gram[s] = exact(panel[s], panel[s], TN)
        strip_here = pl.ds(pl.multiple_of(col * strip, strip), strip)

        upper = col < n_col // 2
        left, right = sides

        def gram_send(other, s=s):
            remote(gram.at[s, strip_here, right], gram_in.at[s, row, :, right], 2, s, on_row(other)).start()

        def gram_send_left(other, s=s):
            remote(gram.at[s, strip_here, left], gram_in.at[s, row, :, left], 10, s, on_row(other)).start()

        others(row, n_row, gram_send)

        @pl.when(upper)
        def _():
            others(row, n_row, gram_send_left)

        gram_in[s, row] = gram[s, strip_here, :]

        panel_parts = split(panel[s])
        for low in range(0, n_cols, LANES):
            high = min(n_cols, low + LANES)
            part = product(split(b[:, low:high]), panel_parts, TN)
            for k in range(2):
                h_part[s, k, low:high, :] = part[:, k * half : (k + 1) * half]
        remote(h_part.at[s, 1 - core], h_in.at[s], 4, s, on_row(row + 1 - 2 * core)).start()

        def piece_of(other):
            return pl.ds(pl.multiple_of(other * piece, 8), piece)

        def h_send(other, s=s):
            remote(h_sum.at[s, piece_of(other)], h_rows.at[s, z], 5, s, on_row(2 * other + core)).start()

        def h_share(other, s=s):
            mine = h_all.at[s, core, piece_of(z)]
            remote(mine, mine, 6, s, on_row(2 * other + core)).start()

        def gram_share(other, s=s):
            block = gram_all.at[s, strip_here, right]
            remote(block, block, 9, s, on_col(other)).start()

        def gram_share_left(other, s=s):
            block = gram_all.at[s, strip_here, left]
            remote(block, block, 3, s, on_col(other)).start()

        arrived(h_in.at[s], 4, s)
        h_sum[s] = h_part[s, core] + h_in[s]
        others(z, n_z, h_send)
        h_rows[s, z] = h_sum[s, piece_of(z), :]

        arrived(gram_in.at[s, pl.ds(0, n_row - 1), :, right], 2, s)
        gram_all[s, strip_here, right] = jnp.sum(gram_in[s, :, :, right], axis=0)
        others(col, n_col, gram_share)

        @pl.when(upper)
        def _(s=s):
            arrived(gram_in.at[s, pl.ds(0, n_row - 1), :, left], 10, s)
            gram_all[s, strip_here, left] = jnp.sum(gram_in[s, :, :, left], axis=0)
            others(col, n_col, gram_share_left)

        table[:, rank:] = jnp.where(
            lax.broadcasted_iota(jnp.int32, (rank, rank), 0) == lax.broadcasted_iota(jnp.int32, (rank, rank), 1), 1.0, 0.0
        )
        arrived(h_rows.at[s, pl.ds(0, n_z - 1)], 5, s)
        h_all[s, core, piece_of(z), :] = jnp.sum(h_rows[s], axis=0)
        others(z, n_z, h_share)

        arrived(gram_all.at[s, pl.ds(0, rank - strip), right], 9, s)

        @pl.when(upper)
        def _(s=s):
            arrived(gram_all.at[s, pl.ds(0, half - strip), left], 3, s)

        @pl.when(jnp.logical_not(upper))
        def _(s=s):
            arrived(gram_all.at[s, pl.ds(0, half), left], 3, s)

        table[:half, :rank] = gram_all[s, :half, :]
        table[half:, half:rank] = gram_all[s, half:, half:]
        eliminate(table, 0)
        eliminate(table, 1)
        arrived(h_all.at[s, 0, pl.ds(0, n_cols - piece)], 6, s)
        remote(h_all.at[s, core], h_all.at[s, core], 8, s, on_row(row + 1 - 2 * core)).start()

        inverse = split(table[:, rank:])
        for low, high in blocks:
            ortho[s, low:high, :] = product(split(panel[s, low:high, :]), inverse, NT)
        thirds = [(low, min(n_cols, low + 192)) for low in range(0, n_cols, 192)]

        def factor_half(k, low, high, s=s):
            side = split(table[:, pl.ds(pl.multiple_of(rank + k * half, LANES), half)])
            rows = split(h_all[s, k, low:high, :])
            return lax.dot_general(
                jnp.concatenate([rows[0], rows[1], rows[0]], axis=1),
                jnp.concatenate([side[1], side[0], side[0]], axis=1),
                NT,
                preferred_element_type=F32,
            )

        for low, high in thirds:
            f[s, low:high, :] = factor_half(core, low, high)
        arrived(h_all.at[s, 0], 8, s)
        for low, high in thirds:
            f[s, low:high, :] = f[s, low:high, :] + factor_half(1 - core, low, high)
        if s == 1:
            squares_send(1)
        right = split(f[s])
        for low, high in blocks:
            b[low:high, :] = b[low:high, :] - 0.05 * product(split(ortho[s, low:high, :]), right, NT)
            if s == 0:
                b[low:high, :] = b[low:high, :] + g[1, low:high, :]
                partial[1, low:high, :] = product(split(b[low:high, :]), right, NN)
        if s == 0:
            panel_send(1)

    momentum_out[...] = b[...]
    scale = scale_of(1)
    weight_step(weight_out, 1, scale, right)
    basis_out[...] = f[1] * scale

    for s in range(2):
        for side, (arrival, spread) in zip(sides, panel_phases):

            @pl.when(col < owners)
            def _(s=s, side=side, arrival=arrival, spread=spread):
                sent(panel_in.at[s, pl.ds(0, owners - 1), :, side], arrival, s)
                sent(panel_in.at[s, pl.ds(0, n_col - 1), :, side], spread, s)

            @pl.when(col >= owners)
            def _(s=s, side=side, arrival=arrival):
                sent(panel_in.at[s, pl.ds(0, owners), :, side], arrival, s)

        sent(gram_in.at[s, pl.ds(0, n_row - 1), :, sides[1]], 2, s)
        sent(gram_all.at[s, pl.ds(0, (n_col - 1) * strip), sides[1]], 9, s)

        @pl.when(col < n_col // 2)
        def _(s=s):
            sent(gram_in.at[s, pl.ds(0, n_row - 1), :, sides[0]], 10, s)
            sent(gram_all.at[s, pl.ds(0, (n_col - 1) * strip), sides[0]], 3, s)

        sent(h_in.at[s], 4, s)
        sent(h_rows.at[s, pl.ds(0, n_z - 1)], 5, s)
        sent(h_rows.at[s, pl.ds(0, n_z - 1)], 6, s)
        sent(squares.at[s, pl.ds(0, n_col - 1)], 7, s)
        sent(h_in.at[s], 8, s)


def solution(mesh):
    n_row, n_col = mesh.shape["row"], mesh.shape["col"]

    def local(weight, momentum, gradients, basis, step):
        (n_rows, n_cols), rank = weight.shape, basis.shape[1]
        owned = -(-n_rows // (8 * n_col)) * 8
        anywhere = pl.BlockSpec(memory_space=pltpu.HBM)
        vmem = functools.partial(pltpu.VMEM, dtype=F32)
        half, n_z = rank // 2, n_row // 2
        return pl.pallas_call(
            functools.partial(kernel, n_cols * n_col, n_row, n_col),
            out_shape=(
                jax.ShapeDtypeStruct(weight.shape, F32),
                jax.ShapeDtypeStruct(weight.shape, F32),
                jax.ShapeDtypeStruct(basis.shape, F32),
            ),
            in_specs=[anywhere] * 4 + [pl.BlockSpec(memory_space=pltpu.SMEM)],
            out_specs=(pl.BlockSpec(memory_space=pltpu.VMEM),) * 3,
            scratch_shapes=[
                vmem((n_rows, n_cols)),
                vmem((n_rows, n_cols)),
                vmem((2, n_rows, n_cols)),
                vmem((n_cols, rank)),
                vmem((n_rows, n_cols)),
                vmem((2, n_rows, rank)),
                vmem((2, n_col, owned, rank)),
                vmem((2, n_rows, rank)),
                vmem((2, rank, rank)),
                vmem((2, n_row, rank // n_col, rank)),
                vmem((2, rank, rank)),
                vmem((rank, 2 * rank)),
                vmem((2, n_rows, rank)),
                vmem((2, 2, n_cols, half)),
                vmem((2, n_cols, half)),
                vmem((2, n_cols, half)),
                vmem((2, n_z, n_cols // n_z, half)),
                vmem((2, 2, n_cols, half)),
                vmem((2, n_cols, rank)),
                vmem((2, n_col, 1, rank)),
                pltpu.SemaphoreType.DMA((5,)),
                pltpu.SemaphoreType.DMA((2, 13)),
                pltpu.SemaphoreType.DMA((2, 13)),
            ],
            compiler_params=pltpu.CompilerParams(collective_id=0, has_side_effects=True, vmem_limit_bytes=54500 * 1024),
        )(weight, momentum, gradients, basis, step)

    return jax.shard_map(
        local,
        mesh=mesh,
        in_specs=(P("row", "col"), P("row", "col"), P(None, "row", "col"), P("col", None), P()),
        out_specs=(P("row", "col"), P("row", "col"), P("col", None)),
        check_vma=False,
    )
```
